32 devices in a mesh: cols: 4 (over y, x), dom: 8 (over z, core).
Axes of the slice: x: 2, y: 2, z: 4, core: 2. Of those that a mesh axis runs over, the one named last changes fastest.
Arguments:
- features: bfloat16 [768, 4096], P('cols', 'dom'), may hold values from -6 to 6
- proj_in: bfloat16 [768, 256], P('cols'), may hold values from -0.3125 to 0.3125
- self_weight: bfloat16 [256, 256], replicated, may hold values from -0.375 to 0.375
- neigh_weight: bfloat16 [256, 256], replicated, may hold values from -0.375 to 0.375
- neighbors: int32 [16, 4096], P(None, 'dom'), may hold values from 0 to 1023, as said below
- degree: int32 [4096], P('dom'), may hold values from 1 to 16
- send_rows: int32 [8, 512], P('dom'), may hold values from 0 to 511
- send_count: int32 [8, 8], P('dom'), may hold values from 0 to 64, as said below
Outputs:
- layer_out: bfloat16 [256, 4096], P('cols', 'dom')
The draws below stay inside these ranges and needn't reach their ends.
Inputs may be any that keep to these rules, and one draw needn't show every extreme that they name: `neighbors`: A code at or above 512 names a source partition other than the node's own and a slot below send_count of that source towards the node's partition. Every partition's rows are received in full (64 slots) from every other partition for at least one partition in every draw. `send_count`: zero on the diagonal; elsewhere 1 to 64, and 64 from every source towards at least one partition.
All inputs are finite; a program needn't handle non-finite values.
Results may differ from the reference program's by a relative error of at most 0.0051.
Values may be sent and summed in bfloat16 or wider, within the bound.
A program may use at most 64 MiB of HBM per device.

```python
import jax
import jax.numpy as jnp
from jax import lax

D_IN = 768
HID = 256
NODE_DEV = 512
K = 16
CAP = 64
NODES = 4096
N_DOM = 8


def shared_counts(key):
    base = jax.random.fold_in(key, 7)
    key_hot, key_pick, key_low = jax.random.split(base, 3)
    hot = jax.random.randint(key_hot, (N_DOM,), 0, 4) == 0
    chosen = jax.random.randint(key_pick, (), 0, N_DOM)
    hot = jnp.logical_or(hot, jnp.arange(N_DOM) == chosen)
    low = jax.random.randint(key_low, (N_DOM, N_DOM), 1, CAP // 2 + 1)
    counts = jnp.where(hot[None, :], CAP, low)
    diagonal = jnp.arange(N_DOM)[:, None] == jnp.arange(N_DOM)[None, :]
    counts = jnp.where(diagonal, 0, counts).astype(jnp.int32)
    return (counts, hot)


def draw_send_count(key, part):
    return shared_counts(key)[0]


def draw_neighbors(key, part):
    counts, hot = shared_counts(key)
    inner = jax.random.fold_in(key, 11)
    key_local, key_roll, key_source, key_slot = jax.random.split(inner, 4)
    part_of = (jnp.arange(NODES) // NODE_DEV)[:, None]
    local = jax.random.randint(key_local, (NODES, K), 0, NODE_DEV)
    roll = jax.random.randint(key_roll, (NODES, K), 0, 8)
    remote = roll < jnp.where(hot[part_of], 4, 1)
    source = (part_of + 1 + jax.random.randint(key_source, (NODES, K), 0, N_DOM - 1)) % N_DOM
    limit = counts[source, part_of]
    slot = jax.random.randint(key_slot, (NODES, K), 0, 1 << 20) % limit
    code = jnp.where(remote, NODE_DEV + source * CAP + slot, local)
    return code.T.astype(jnp.int32)


def with_ends(result, rng, smallest, top_value):
    extent = result.shape
    place = [jax.random.randint(jax.random.fold_in(rng, axis), (), 0, extent[axis]) for axis in range(len(extent))]
    result = result.at[tuple(place)].set(smallest)
    longest = extent.index(max(extent))
    place[longest] = (place[longest] + 1) % extent[longest]
    return result.at[tuple(place)].set(top_value)


def strengthened(entries, stream_key, source, target, shards_of, factor):
    owner, partner = [(jnp.arange(entries.shape[axis_at]) // (entries.shape[axis_at] // shards_of)).reshape([-1 if axis == axis_at else 1 for axis in range(entries.ndim)]) for axis_at in (source, target)]
    chosen = jax.random.permutation(stream_key, shards_of)[partner]
    strong = (owner == chosen) | (owner == (partner + shards_of // 2) % shards_of)
    return jnp.where(strong, factor * entries, entries)


def level_of(stream_key, shape, shards, least, high):
    gain = 1.0
    for axis_at, blocks in shards:
        heights = jax.random.uniform(jax.random.fold_in(jax.random.fold_in(stream_key, 6), axis_at), (blocks,), jnp.float32, least / len(shards), high / len(shards))
        gain = gain * jnp.repeat(jnp.exp(heights), shape[axis_at] // blocks).reshape((-1,) + (1,) * (len(shape) - 1 - axis_at))
    return gain


def noise(own_key, dims, deviation, most, cuts=(), kind=jnp.bfloat16):
    drawn = deviation * jax.random.normal(own_key, dims, jnp.float32)
    if cuts:
        drawn = drawn * level_of(own_key, dims, cuts, -0.22, 0.18)
    return jnp.clip(drawn, -most, most).astype(kind)


def bell_draw_with(stream_key, dims, width, reach, cuts, heavy, held_as=jnp.bfloat16):
    array = width * jax.random.normal(stream_key, dims, jnp.float32)
    if cuts:
        array = array * level_of(stream_key, dims, cuts, -0.22, 0.18)
    return jnp.clip(strengthened(array, jax.random.fold_in(stream_key, 3), *heavy), -reach, reach).astype(held_as)


def setup_inputs(seed: int = 0) -> dict:
    streams_of = jax.random.split(jax.random.key(seed), 9)
    features = noise(streams_of[0], (D_IN, NODES), 1.0, 6.0, ((0, 4), (1, 8)))
    proj_in = bell_draw_with(streams_of[1], (D_IN, HID), D_IN ** -0.5, 0.3125, ((0, 4),), (0, 1, 4, 2.0))
    self_weight = noise(streams_of[2], (HID, HID), HID ** -0.5, 0.375)
    neigh_weight = noise(streams_of[3], (HID, HID), HID ** -0.5, 0.375)
    neighbors = draw_neighbors(jax.random.fold_in(streams_of[8], 71), 0)
    degree = with_ends(jax.random.randint(streams_of[5], (NODES,), 1, K + 1), jax.random.fold_in(streams_of[5], 1), 1, K).astype(jnp.int32)
    send_rows = with_ends(jax.random.randint(streams_of[6], (N_DOM, N_DOM * CAP), 0, NODE_DEV), jax.random.fold_in(streams_of[6], 1), 0, NODE_DEV - 1).astype(jnp.int32)
    send_count = draw_send_count(jax.random.fold_in(streams_of[8], 71), 0)
    return dict(features=features, proj_in=proj_in, self_weight=self_weight, neigh_weight=neigh_weight, neighbors=neighbors, degree=degree, send_rows=send_rows, send_count=send_count)


def reference(features, proj_in, self_weight, neigh_weight, neighbors, degree, send_rows, send_count):
    hidden = jnp.dot(features.T, proj_in, preferred_element_type=jnp.float32).astype(jnp.bfloat16)
    codes = neighbors.T.reshape(N_DOM, NODE_DEV, K)
    degs = degree.reshape(N_DOM, NODE_DEV)
    parts = jnp.arange(N_DOM, dtype=jnp.int32)

    def one_part(inputs):
        code, deg, part = inputs
        remote = code >= NODE_DEV
        rel = jnp.maximum(code - NODE_DEV, 0)
        source = rel // CAP
        slot = rel % CAP
        sent = send_rows[source, part * CAP + slot]
        valid = slot < send_count[source, part]
        rows = jnp.where(remote, source * NODE_DEV + sent, part * NODE_DEV + code).astype(jnp.int32)
        used = jnp.arange(K, dtype=jnp.int32)[None, :] < deg[:, None]
        keep = jnp.logical_and(used, jnp.logical_or(jnp.logical_not(remote), valid))
        picked = hidden[rows].astype(jnp.float32)
        total = jnp.sum(jnp.where(keep[:, :, None], picked, jnp.float32(0.0)), axis=1)
        return (total / deg[:, None].astype(jnp.float32)).astype(jnp.bfloat16)

    mean = lax.map(one_part, (codes, degs, parts)).reshape(NODES, HID)
    total = jnp.dot(hidden, self_weight, preferred_element_type=jnp.float32)
    total = total + jnp.dot(mean, neigh_weight, preferred_element_type=jnp.float32)
    return jnp.maximum(total, 0.0).astype(jnp.bfloat16).T
```

```python
import functools
import math

import jax
import jax.numpy as jnp
from jax import lax
from jax.experimental import pallas as pl
from jax.experimental.pallas import tpu as pltpu
from jax.sharding import PartitionSpec as P

MESH = pl.DeviceIdType.MESH
LANES = 128


def dot(left, right, left_dim, right_dim):
    return lax.dot_general(
        left, right, (((left_dim,), (right_dim,)), ((), ())), preferred_element_type=jnp.float32
    )


def kernel(
    cols,
    parts,
    capacity,
    feat_hbm,
    proj_hbm,
    selfw_hbm,
    neighw_hbm,
    neigh_hbm,
    degree_hbm,
    rows_hbm,
    count_hbm,
    out_ref,
    feat,
    proj,
    selfw,
    neighw,
    neigh,
    degree,
    rows,
    count,
    own,
    outgoing_sum,
    incoming_sum,
    hidden_all,
    mean_all,
    pick,
    packed_out,
    packed_in,
    table,
    counts,
    in_sem,
    sum_send,
    sum_recv,
    row_send,
    row_recv,
    hid_send,
    hid_recv,
    mean_send,
    mean_recv,
):
    column = lax.axis_index("cols")
    part = lax.axis_index("dom")
    width = out_ref.shape[0]
    nodes = out_ref.shape[1]
    hid = width * cols
    slots = rows.shape[1]
    slot_count = neigh.shape[0]
    fold = LANES // capacity
    short = width // fold

    loads = [
        pltpu.make_async_copy(source, target, in_sem.at[i])
        for i, (source, target) in enumerate(
            (
                (feat_hbm, feat),
                (proj_hbm, proj),
                (rows_hbm, rows),
                (count_hbm, count),
                (neigh_hbm, neigh),
                (degree_hbm, degree),
                (selfw_hbm, selfw),
                (neighw_hbm, neighw),
            )
        )
    ]
    for load in loads:
        load.start()

    barrier = pltpu.get_barrier_semaphore()
    for step in range(1, cols):
        pl.semaphore_signal(
            barrier, inc=1, device_id=((column + step) % cols, part), device_id_type=MESH
        )

    def greet(step, carry):
        pl.semaphore_signal(
            barrier, inc=1, device_id=(column, (part + step) % parts), device_id_type=MESH
        )
        return carry

    lax.fori_loop(1, parts, greet, 0)

    loads[0].wait()
    loads[1].wait()
    partial_value = dot(proj[...], feat[...], 0, 0)
    own[...] = partial_value
    outgoing_sum[...] = partial_value.astype(outgoing_sum.dtype)
    pl.semaphore_wait(barrier, cols + parts - 2)

    def band(index):
        return pl.ds(pl.multiple_of(index * width, width), width)

    def to_column(source, target, send, recv, step):
        peer = (column + step) % cols
        return pltpu.make_async_remote_copy(
            src_ref=source,
            dst_ref=target,
            send_sem=send.at[step - 1],
            recv_sem=recv.at[step - 1],
            device_id=(peer, part),
            device_id_type=MESH,
        )

    sums = [
        to_column(
            outgoing_sum.at[band((column + step) % cols)],
            incoming_sum.at[step - 1],
            sum_send,
            sum_recv,
            step,
        )
        for step in range(1, cols)
    ]
    for copy in sums:
        copy.start()

    for load in loads[2:]:
        load.wait()
    group = min(slots, 512)
    spread = group * fold

    def choose(index, carry):
        start = pl.multiple_of(index * group, group)
        wanted = rows[:, pl.ds(start, group)]
        source = (
            lax.broadcasted_iota(jnp.int32, (parts, group), 1) + start
        ) // capacity == lax.broadcasted_iota(jnp.int32, (parts, group), 0)
        amount = dot(
            jnp.broadcast_to(count[...].astype(jnp.float32), (8, parts)).astype(jnp.bfloat16),
            source.astype(jnp.float32).astype(jnp.bfloat16),
            1,
            0,
        )[0:1, :]
        slot = (lax.broadcasted_iota(jnp.int32, (1, group), 1) % capacity).astype(jnp.float32)
        wanted = jnp.where(slot < amount, wanted, -1)
        pieces = []
        for block in range(group // capacity):
            piece = wanted[:, block * capacity : (block + 1) * capacity]
            pieces += [piece] * fold
        wide = jnp.concatenate(pieces, axis=1)
        hit = lax.broadcasted_iota(jnp.int32, (nodes, spread), 0) == wide
        pick[:, pl.ds(pl.multiple_of(index * spread, spread), spread)] = jnp.where(
            hit, 1.0, 0.0
        ).astype(jnp.bfloat16)
        return carry

    lax.fori_loop(0, slots // group, choose, 0)

    used = lax.broadcasted_iota(jnp.int32, (slot_count, nodes), 0) < degree[...]
    codes = jnp.where(used, neigh[...], -1)
    neigh[...] = codes
    depth = 256
    row_of = lax.broadcasted_iota(jnp.int32, (depth, LANES), 0).astype(jnp.float32).astype(jnp.bfloat16)
    one = jnp.ones((depth, LANES), jnp.bfloat16)
    zero = jnp.zeros((depth, LANES), jnp.bfloat16)

    def tally(index, carry):
        start = pl.multiple_of(index * depth, depth)
        for lane in range(nodes // LANES):
            there = slice(lane * LANES, (lane + 1) * LANES)
            near = jnp.clip(neigh[:, there] - start, -1, depth).astype(jnp.float32)
            total = zero
            for slot in range(slot_count):
                code = jnp.broadcast_to(near[slot : slot + 1, :], (16, LANES)).astype(jnp.bfloat16)
                code = jnp.concatenate([code] * (depth // 16), axis=0)
                total = total + jnp.where(row_of == code, one, zero)
            counts[pl.ds(start, depth), there] = total
        return carry

    lax.fori_loop(0, counts.shape[0] // depth, tally, 0)

    mine = (
        lax.broadcasted_iota(jnp.int32, (width, hid), 0) + column * width
        == lax.broadcasted_iota(jnp.int32, (width, hid), 1)
    )
    mine = jnp.where(mine, 1.0, 0.0).astype(jnp.bfloat16)
    self_rows = dot(mine, selfw[...], 1, 1).astype(jnp.bfloat16)
    neigh_rows = dot(mine, neighw[...], 1, 1).astype(jnp.bfloat16)

    total = own[band(column), :]
    for step in range(1, cols):
        sums[step - 1].wait_recv()
    for step in range(1, cols):
        total = total + incoming_sum[step - 1].astype(jnp.float32)
    hidden = total.astype(jnp.bfloat16)
    hidden_all[band(column), :] = hidden

    folded = lax.broadcasted_iota(jnp.int32, (short, spread), 1) % LANES // capacity

    def pack(index, carry):
        start = pl.multiple_of(index * spread, spread)
        chosen = dot(hidden_all[band(column), :], pick[:, pl.ds(start, spread)], 1, 0)
        tight = chosen[0:short, :]
        for piece in range(1, fold):
            tight = jnp.where(folded == piece, chosen[piece * short : (piece + 1) * short, :], tight)
        tight = tight.astype(jnp.bfloat16)
        for block in range(spread // LANES):
            packed_out[index * (spread // LANES) + block] = tight[:, block * LANES : (block + 1) * LANES]
        return carry

    lax.fori_loop(0, slots // group, pack, 0)

    def to_part(step):
        peer = (part + step) % parts
        return pltpu.make_async_remote_copy(
            src_ref=packed_out.at[peer],
            dst_ref=packed_in.at[part],
            send_sem=row_send.at[step],
            recv_sem=row_recv.at[step],
            device_id=(column, peer),
            device_id_type=MESH,
        )

    def send_rows(step, carry):
        to_part(step).start()
        return carry

    lax.fori_loop(1, parts, send_rows, 0)

    def share(buffer, send, recv):
        return [
            to_column(buffer.at[band(column)], buffer.at[band(column)], send, recv, step)
            for step in range(1, cols)
        ]

    hidden_copies = share(hidden_all, hid_send, hid_recv)
    for copy in hidden_copies:
        copy.start()

    packed_in[part] = jnp.zeros((short, LANES), jnp.bfloat16)
    local_sum = dot(hidden, counts[0:nodes, :], 1, 0)

    def arrive(step, carry):
        to_part(step).wait_recv()
        return carry

    lax.fori_loop(1, parts, arrive, 0)

    half = lax.broadcasted_iota(jnp.int32, (short, LANES), 1) // capacity

    def unpack(index, carry):
        for piece in range(fold):
            value = jnp.zeros((short, LANES), jnp.float32)
            for place in range(fold):
                block = packed_in[index * fold + place].astype(jnp.float32)
                shift = (place - piece) * capacity % LANES
                if shift:
                    block = pltpu.roll(block, shift, 1)
                value = jnp.where(half == place, block, value)
            table[piece * short : (piece + 1) * short, pl.ds(pl.multiple_of(index * LANES, LANES), LANES)] = (
                value.astype(jnp.bfloat16)
            )
        return carry

    lax.fori_loop(0, parts // fold, unpack, 0)
    summed = local_sum + dot(table[...], counts[nodes:, :], 1, 0)
    mean_all[band(column), :] = (summed / degree[...].astype(jnp.float32)).astype(jnp.bfloat16)
    mean_copies = share(mean_all, mean_send, mean_recv)
    for copy in mean_copies:
        copy.start()
    for copy in hidden_copies:
        copy.wait_recv()
    result = dot(self_rows, hidden_all[...], 1, 0)
    for copy in mean_copies:
        copy.wait_recv()
    result = result + dot(neigh_rows, mean_all[...], 1, 0)
    out_ref[...] = jnp.maximum(result, 0.0).astype(out_ref.dtype)

    for copy in sums + hidden_copies + mean_copies:
        copy.wait_send()

    def sent(step, carry):
        to_part(step).wait_send()
        return carry

    lax.fori_loop(1, parts, sent, 0)


def local(features, proj_in, self_weight, neigh_weight, neighbors, degree, send_rows, send_count):
    cols = lax.axis_size("cols")
    parts = lax.axis_size("dom")
    hid = proj_in.shape[1]
    width = hid // cols
    nodes = features.shape[1]
    slots = send_rows.shape[1]
    capacity = slots // parts
    fold = LANES // capacity
    short = width // fold
    degree = degree.reshape(1, nodes)
    arguments = (
        features,
        proj_in,
        self_weight,
        neigh_weight,
        neighbors,
        degree,
        send_rows,
        send_count,
    )
    bf16 = jnp.bfloat16
    copies = pltpu.SemaphoreType.DMA
    return pl.pallas_call(
        functools.partial(kernel, cols, parts, capacity),
        out_shape=jax.ShapeDtypeStruct((width, nodes), bf16),
        in_specs=[pl.BlockSpec(memory_space=pl.ANY)] * len(arguments),
        out_specs=pl.BlockSpec(memory_space=pltpu.VMEM),
        scratch_shapes=[pltpu.VMEM(a.shape, a.dtype) for a in arguments]
        + [
            pltpu.VMEM((hid, nodes), jnp.float32),
            pltpu.VMEM((hid, nodes), bf16),
            pltpu.VMEM((cols - 1, width, nodes), bf16),
            pltpu.VMEM((hid, nodes), bf16),
            pltpu.VMEM((hid, nodes), bf16),
            pltpu.VMEM((nodes, slots * fold), bf16),
            pltpu.VMEM((parts, short, LANES), bf16),
            pltpu.VMEM((parts, short, LANES), bf16),
            pltpu.VMEM((width, slots), bf16),
            pltpu.VMEM((nodes + slots, nodes), bf16),
            copies((len(arguments),)),
            copies((cols - 1,)),
            copies((cols - 1,)),
            copies((parts,)),
            copies((parts,)),
            copies((cols - 1,)),
            copies((cols - 1,)),
            copies((cols - 1,)),
            copies((cols - 1,)),
        ],
        compiler_params=pltpu.CompilerParams(
            collective_id=0, has_side_effects=True, vmem_limit_bytes=48 * 1024 * 1024
        ),
        name="layer",
    )(*arguments)


def solution(mesh):
    return jax.shard_map(
        local,
        mesh=mesh,
        in_specs=(
            P("cols", "dom"),
            P("cols", None),
            P(),
            P(),
            P(None, "dom"),
            P("dom"),
            P("dom", None),
            P("dom", None),
        ),
        out_specs=P("cols", "dom"),
        check_vma=False,
    )
```

```python
import functools
import math

import jax
import jax.numpy as jnp
from jax import lax
from jax.experimental import pallas as pl
from jax.experimental.pallas import tpu as pltpu
from jax.sharding import PartitionSpec as P

MESH = pl.DeviceIdType.MESH
LANES = 128


def dot(left, right, left_dim, right_dim):
    return lax.dot_general(
        left, right, (((left_dim,), (right_dim,)), ((), ())), preferred_element_type=jnp.float32
    )


def kernel(
    cols,
    parts,
    capacity,
    feat_hbm,
    proj_hbm,
    selfw_hbm,
    neighw_hbm,
    neigh_hbm,
    degree_hbm,
    rows_hbm,
    count_hbm,
    out_ref,
    feat,
    proj,
    selfw,
    neighw,
    neigh,
    degree,
    rows,
    count,
    own,
    outgoing_sum,
    incoming_sum,
    hidden_all,
    mean_all,
    pick,
    packed_out,
    packed_in,
    table,
    counts,
    in_sem,
    sum_send,
    sum_recv,
    row_send,
    row_recv,
    hid_send,
    hid_recv,
    mean_send,
    mean_recv,
):
    column = lax.axis_index("cols")
    part = lax.axis_index("dom")
    width = out_ref.shape[0]
    nodes = out_ref.shape[1]
    hid = width * cols
    slots = rows.shape[1]
    slot_count = neigh.shape[0]
    fold = LANES // capacity
    short = width // fold

    loads = [
        pltpu.make_async_copy(source, target, in_sem.at[i])
        for i, (source, target) in enumerate(
            (
                (feat_hbm, feat),
                (proj_hbm, proj),
                (rows_hbm, rows),
                (count_hbm, count),
                (neigh_hbm, neigh),
                (degree_hbm, degree),
                (selfw_hbm, selfw),
                (neighw_hbm, neighw),
            )
        )
    ]
    for load in loads:
        load.start()

    barrier = pltpu.get_barrier_semaphore()
    for step in range(1, cols):
        pl.semaphore_signal(
            barrier, inc=1, device_id=((column + step) % cols, part), device_id_type=MESH
        )

    def greet(step, carry):
        pl.semaphore_signal(
            barrier, inc=1, device_id=(column, (part + step) % parts), device_id_type=MESH
        )
        return carry

    lax.fori_loop(1, parts, greet, 0)

    loads[0].wait()
    loads[1].wait()
    partial_value = dot(proj[...], feat[...], 0, 0)
    own[...] = partial_value
    outgoing_sum[...] = partial_value.astype(outgoing_sum.dtype)
    pl.semaphore_wait(barrier, cols + parts - 2)

    def band(index):
        return pl.ds(pl.multiple_of(index * width, width), width)

    def to_column(source, target, send, recv, step):
        peer = (column + step) % cols
        return pltpu.make_async_remote_copy(
            src_ref=source,
            dst_ref=target,
            send_sem=send.at[step - 1],
            recv_sem=recv.at[step - 1],
            device_id=(peer, part),
            device_id_type=MESH,
        )

    sums = [
        to_column(
            outgoing_sum.at[band((column + step) % cols)],
            incoming_sum.at[step - 1],
            sum_send,
            sum_recv,
            step,
        )
        for step in range(1, cols)
    ]
    for copy in sums:
        copy.start()

    for load in loads[2:]:
        load.wait()
    group = min(slots, 512)
    spread = group * fold

    def choose(index, carry):
        start = pl.multiple_of(index * group, group)
        wanted = rows[:, pl.ds(start, group)]
        source = (
            lax.broadcasted_iota(jnp.int32, (parts, group), 1) + start
        ) // capacity == lax.broadcasted_iota(jnp.int32, (parts, group), 0)
        amount = dot(
            jnp.broadcast_to(count[...].astype(jnp.float32), (8, parts)).astype(jnp.bfloat16),
            source.astype(jnp.float32).astype(jnp.bfloat16),
            1,
            0,
        )[0:1, :]
        slot = (lax.broadcasted_iota(jnp.int32, (1, group), 1) % capacity).astype(jnp.float32)
        wanted = jnp.where(slot < amount, wanted, -1)
        pieces = []
        for block in range(group // capacity):
            piece = wanted[:, block * capacity : (block + 1) * capacity]
            pieces += [piece] * fold
        wide = jnp.concatenate(pieces, axis=1)
        hit = lax.broadcasted_iota(jnp.int32, (nodes, spread), 0) == wide
        pick[:, pl.ds(pl.multiple_of(index * spread, spread), spread)] = jnp.where(
            hit, 1.0, 0.0
        ).astype(jnp.bfloat16)
        return carry

    lax.fori_loop(0, slots // group, choose, 0)

    used = lax.broadcasted_iota(jnp.int32, (slot_count, nodes), 0) < degree[...]
    codes = jnp.where(used, neigh[...], -1)
    neigh[...] = codes
    depth = 256
    row_of = lax.broadcasted_iota(jnp.int32, (depth, LANES), 0).astype(jnp.float32).astype(jnp.bfloat16)
    one = jnp.ones((depth, LANES), jnp.bfloat16)
    zero = jnp.zeros((depth, LANES), jnp.bfloat16)

    def tally(index, carry):
        start = pl.multiple_of(index * depth, depth)
        for lane in range(nodes // LANES):
            there = slice(lane * LANES, (lane + 1) * LANES)
            near = jnp.clip(neigh[:, there] - start, -1, depth).astype(jnp.float32)
            total = zero
            for slot in range(slot_count):
                code = jnp.broadcast_to(near[slot : slot + 1, :], (16, LANES)).astype(jnp.bfloat16)
                code = jnp.concatenate([code] * (depth // 16), axis=0)
                total = total + jnp.where(row_of == code, one, zero)
            counts[pl.ds(start, depth), there] = total
        return carry

    lax.fori_loop(0, counts.shape[0] // depth, tally, 0)

    mine = (
        lax.broadcasted_iota(jnp.int32, (width, hid), 0) + column * width
        == lax.broadcasted_iota(jnp.int32, (width, hid), 1)
    )
    mine = jnp.where(mine, 1.0, 0.0).astype(jnp.bfloat16)
    self_rows = dot(mine, selfw[...], 1, 1).astype(jnp.bfloat16)
    neigh_rows = dot(mine, neighw[...], 1, 1).astype(jnp.bfloat16)

    total = own[band(column), :]
    for step in range(1, cols):
        sums[step - 1].wait_recv()
    for step in range(1, cols):
        total = total + incoming_sum[step - 1].astype(jnp.float32)
    hidden = total.astype(jnp.bfloat16)
    hidden_all[band(column), :] = hidden

    folded = lax.broadcasted_iota(jnp.int32, (short, spread), 1) % LANES // capacity

    def pack(index, carry):
        start = pl.multiple_of(index * spread, spread)
        chosen = dot(hidden_all[band(column), :], pick[:, pl.ds(start, spread)], 1, 0)
        tight = chosen[0:short, :]
        for piece in range(1, fold):
            tight = jnp.where(folded == piece, chosen[piece * short : (piece + 1) * short, :], tight)
        tight = tight.astype(jnp.bfloat16)
        for block in range(spread // LANES):
            packed_out[index * (spread // LANES) + block] = tight[:, block * LANES : (block + 1) * LANES]
        return carry

    lax.fori_loop(0, slots // group, pack, 0)

    def to_part(step):
        peer = (part + step) % parts
        return pltpu.make_async_remote_copy(
            src_ref=packed_out.at[peer],
            dst_ref=packed_in.at[part],
            send_sem=row_send.at[step],
            recv_sem=row_recv.at[step],
            device_id=(column, peer),
            device_id_type=MESH,
        )

    def send_rows(step, carry):
        to_part(step).start()
        return carry

    lax.fori_loop(1, parts, send_rows, 0)

    def share(buffer, send, recv):
        return [
            to_column(buffer.at[band(column)], buffer.at[band(column)], send, recv, step)
            for step in range(1, cols)
        ]

    hidden_copies = share(hidden_all, hid_send, hid_recv)
    for copy in hidden_copies:
        copy.start()

    packed_in[part] = jnp.zeros((short, LANES), jnp.bfloat16)
    local_sum = dot(hidden, counts[0:nodes, :], 1, 0)

    def arrive(step, carry):
        to_part(step).wait_recv()
        return carry

    lax.fori_loop(1, parts, arrive, 0)

    half = lax.broadcasted_iota(jnp.int32, (short, LANES), 1) // capacity

    def unpack(index, carry):
        for piece in range(fold):
            value = jnp.zeros((short, LANES), jnp.float32)
            for place in range(fold):
                block = packed_in[index * fold + place].astype(jnp.float32)
                shift = (place - piece) * capacity % LANES
                if shift:
                    block = pltpu.roll(block, shift, 1)
                value = jnp.where(half == place, block, value)
            table[piece * short : (piece + 1) * short, pl.ds(pl.multiple_of(index * LANES, LANES), LANES)] = (
                value.astype(jnp.bfloat16)
            )
        return carry

    lax.fori_loop(0, parts // fold, unpack, 0)
    summed = local_sum + dot(table[...], counts[nodes:, :], 1, 0)
    mean_all[band(column), :] = (summed / degree[...].astype(jnp.float32)).astype(jnp.bfloat16)
    mean_copies = share(mean_all, mean_send, mean_recv)
    for copy in mean_copies:
        copy.start()
    for copy in hidden_copies:
        copy.wait_recv()
    result = dot(self_rows, hidden_all[...], 1, 0)
    for copy in mean_copies:
        copy.wait_recv()
    result = result + dot(neigh_rows, mean_all[...], 1, 0)
    out_ref[...] = jnp.maximum(result, 0.0).astype(out_ref.dtype)

    for copy in sums + hidden_copies + mean_copies:
        copy.wait_send()

    def sent(step, carry):
        to_part(step).wait_send()
        return carry

    lax.fori_loop(1, parts, sent, 0)


def local(features, proj_in, self_weight, neigh_weight, neighbors, degree, send_rows, send_count):
    cols = lax.axis_size("cols")
    parts = lax.axis_size("dom")
    hid = proj_in.shape[1]
    width = hid // cols
    nodes = features.shape[1]
    slots = send_rows.shape[1]
    capacity = slots // parts
    fold = LANES // capacity
    short = width // fold
    degree = degree.reshape(1, nodes)
    arguments = (
        features,
        proj_in,
        self_weight,
        neigh_weight,
        neighbors,
        degree,
        send_rows,
        send_count,
    )
    bf16 = jnp.bfloat16
    copies = pltpu.SemaphoreType.DMA
    return pl.pallas_call(
        functools.partial(kernel, cols, parts, capacity),
        out_shape=jax.ShapeDtypeStruct((width, nodes), bf16),
        in_specs=[pl.BlockSpec(memory_space=pltpu.HBM)] * len(arguments),
        out_specs=pl.BlockSpec(memory_space=pltpu.VMEM),
        scratch_shapes=[pltpu.VMEM(a.shape, a.dtype) for a in arguments]
        + [
            pltpu.VMEM((hid, nodes), jnp.float32),
            pltpu.VMEM((hid, nodes), bf16),
            pltpu.VMEM((cols - 1, width, nodes), bf16),
            pltpu.VMEM((hid, nodes), bf16),
            pltpu.VMEM((hid, nodes), bf16),
            pltpu.VMEM((nodes, slots * fold), bf16),
            pltpu.VMEM((parts, short, LANES), bf16),
            pltpu.VMEM((parts, short, LANES), bf16),
            pltpu.VMEM((width, slots), bf16),
            pltpu.VMEM((nodes + slots, nodes), bf16),
            copies((len(arguments),)),
            copies((cols - 1,)),
            copies((cols - 1,)),
            copies((parts,)),
            copies((parts,)),
            copies((cols - 1,)),
            copies((cols - 1,)),
            copies((cols - 1,)),
            copies((cols - 1,)),
        ],
        compiler_params=pltpu.CompilerParams(
            collective_id=0, has_side_effects=True, vmem_limit_bytes=67043328
        ),
        name="layer",
    )(*arguments)


def solution(mesh):
    return jax.shard_map(
        local,
        mesh=mesh,
        in_specs=(
            P("cols", "dom"),
            P("cols", None),
            P(),
            P(),
            P(None, "dom"),
            P("dom"),
            P("dom", None),
            P("dom", None),
        ),
        out_specs=P("cols", "dom"),
        check_vma=False,
    )
```

```python
import functools
import math

import jax
import jax.numpy as jnp
from jax import lax
from jax.experimental import pallas as pl
from jax.experimental.pallas import tpu as pltpu
from jax.sharding import PartitionSpec as P

MESH = pl.DeviceIdType.MESH
LANES = 128


def dot(left, right, left_dim, right_dim):
    return lax.dot_general(
        left, right, (((left_dim,), (right_dim,)), ((), ())), preferred_element_type=jnp.float32
    )


def kernel(
    cols,
    parts,
    capacity,
    feat_hbm,
    proj_hbm,
    selfw_hbm,
    neighw_hbm,
    neigh_hbm,
    degree_hbm,
    rows_hbm,
    count_hbm,
    out_ref,
    feat,
    proj,
    selfw,
    neighw,
    neigh,
    degree,
    rows,
    count,
    own,
    outgoing_sum,
    incoming_sum,
    hidden_all,
    mean_all,
    pick,
    packed_out,
    packed_in,
    table,
    counts,
    in_sem,
    sum_send,
    sum_recv,
    row_send,
    row_recv,
    hid_send,
    hid_recv,
    mean_send,
    mean_recv,
):
    column = lax.axis_index("cols")
    part = lax.axis_index("dom")
    width = out_ref.shape[0]
    nodes = out_ref.shape[1]
    hid = width * cols
    slots = rows.shape[1]
    slot_count = neigh.shape[0]
    fold = LANES // capacity
    short = width // fold

    loads = [
        pltpu.make_async_copy(source, target, in_sem.at[i])
        for i, (source, target) in enumerate(
            (
                (feat_hbm, feat),
                (proj_hbm, proj),
                (rows_hbm, rows),
                (count_hbm, count),
                (neigh_hbm, neigh),
                (degree_hbm, degree),
                (selfw_hbm, selfw),
                (neighw_hbm, neighw),
            )
        )
    ]
    for load in loads:
        load.start()

    barrier = pltpu.get_barrier_semaphore()
    for step in range(1, cols):
        pl.semaphore_signal(
            barrier, inc=1, device_id=((column + step) % cols, part), device_id_type=MESH
        )

    def greet(step, carry):
        pl.semaphore_signal(
            barrier, inc=1, device_id=(column, (part + step) % parts), device_id_type=MESH
        )
        return carry

    lax.fori_loop(1, parts, greet, 0)

    loads[0].wait()
    loads[1].wait()
    partial_value = dot(proj[...], feat[...], 0, 0)
    own[...] = partial_value
    outgoing_sum[...] = partial_value.astype(outgoing_sum.dtype)
    pl.semaphore_wait(barrier, cols + parts - 2)

    def band(index):
        return pl.ds(pl.multiple_of(index * width, width), width)

    def to_column(source, target, send, recv, step):
        peer = (column + step) % cols
        return pltpu.make_async_remote_copy(
            src_ref=source,
            dst_ref=target,
            send_sem=send.at[step - 1],
            recv_sem=recv.at[step - 1],
            device_id=(peer, part),
            device_id_type=MESH,
        )

    sums = [
        to_column(
            outgoing_sum.at[band((column + step) % cols)],
            incoming_sum.at[step - 1],
            sum_send,
            sum_recv,
            step,
        )
        for step in range(1, cols)
    ]
    for copy in sums:
        copy.start()

    for load in loads[2:6]:
        load.wait()
    group = min(slots, 512)
    spread = group * fold

    def choose(index, carry):
        start = pl.multiple_of(index * group, group)
        wanted = rows[:, pl.ds(start, group)]
        source = (
            lax.broadcasted_iota(jnp.int32, (parts, group), 1) + start
        ) // capacity == lax.broadcasted_iota(jnp.int32, (parts, group), 0)
        amount = dot(
            jnp.broadcast_to(count[...].astype(jnp.float32), (8, parts)).astype(jnp.bfloat16),
            source.astype(jnp.float32).astype(jnp.bfloat16),
            1,
            0,
        )[0:1, :]
        slot = (lax.broadcasted_iota(jnp.int32, (1, group), 1) % capacity).astype(jnp.float32)
        wanted = jnp.where(slot < amount, wanted, -1)
        pieces = []
        for block in range(group // capacity):
            piece = wanted[:, block * capacity : (block + 1) * capacity]
            pieces += [piece] * fold
        wide = jnp.concatenate(pieces, axis=1)
        hit = lax.broadcasted_iota(jnp.int32, (nodes, spread), 0) == wide
        pick[:, pl.ds(pl.multiple_of(index * spread, spread), spread)] = jnp.where(
            hit, 1.0, 0.0
        ).astype(jnp.bfloat16)
        return carry

    lax.fori_loop(0, slots // group, choose, 0)

    used = lax.broadcasted_iota(jnp.int32, (slot_count, nodes), 0) < degree[...]
    codes = jnp.where(used, neigh[...], -1)
    neigh[...] = codes
    depth = 256
    row_of = lax.broadcasted_iota(jnp.int32, (depth, LANES), 0).astype(jnp.float32).astype(jnp.bfloat16)
    one = jnp.ones((depth, LANES), jnp.bfloat16)
    zero = jnp.zeros((depth, LANES), jnp.bfloat16)

    def tally(index, carry):
        start = pl.multiple_of(index * depth, depth)
        for lane in range(nodes // LANES):
            there = slice(lane * LANES, (lane + 1) * LANES)
            near = jnp.clip(neigh[:, there] - start, -1, depth).astype(jnp.float32)
            total = zero
            for slot in range(slot_count):
                code = jnp.broadcast_to(near[slot : slot + 1, :], (16, LANES)).astype(jnp.bfloat16)
                code = jnp.concatenate([code] * (depth // 16), axis=0)
                total = total + jnp.where(row_of == code, one, zero)
            counts[pl.ds(start, depth), there] = total
        return carry

    lax.fori_loop(0, nodes // depth, tally, 0)

    total = own[band(column), :]
    for step in range(1, cols):
        sums[step - 1].wait_recv()
    for step in range(1, cols):
        total = total + incoming_sum[step - 1].astype(jnp.float32)
    hidden = total.astype(jnp.bfloat16)
    hidden_all[band(column), :] = hidden

    folded = lax.broadcasted_iota(jnp.int32, (short, spread), 1) % LANES // capacity

    def pack(index, carry):
        start = pl.multiple_of(index * spread, spread)
        chosen = dot(hidden_all[band(column), :], pick[:, pl.ds(start, spread)], 1, 0)
        tight = chosen[0:short, :]
        for piece in range(1, fold):
            tight = jnp.where(folded == piece, chosen[piece * short : (piece + 1) * short, :], tight)
        tight = tight.astype(jnp.bfloat16)
        for block in range(spread // LANES):
            packed_out[index * (spread // LANES) + block] = tight[:, block * LANES : (block + 1) * LANES]
        return carry

    lax.fori_loop(0, slots // group, pack, 0)

    def to_part(step):
        peer = (part + step) % parts
        return pltpu.make_async_remote_copy(
            src_ref=packed_out.at[peer],
            dst_ref=packed_in.at[part],
            send_sem=row_send.at[step],
            recv_sem=row_recv.at[step],
            device_id=(column, peer),
            device_id_type=MESH,
        )

    def send_rows(step, carry):
        to_part(step).start()
        return carry

    lax.fori_loop(1, parts, send_rows, 0)

    def share(buffer, send, recv):
        return [
            to_column(buffer.at[band(column)], buffer.at[band(column)], send, recv, step)
            for step in range(1, cols)
        ]

    hidden_copies = share(hidden_all, hid_send, hid_recv)
    for copy in hidden_copies:
        copy.start()

    packed_in[part] = jnp.zeros((short, LANES), jnp.bfloat16)
    lax.fori_loop(nodes // depth, counts.shape[0] // depth, tally, 0)
    for load in loads[6:]:
        load.wait()
    mine = (
        lax.broadcasted_iota(jnp.int32, (width, hid), 0) + column * width
        == lax.broadcasted_iota(jnp.int32, (width, hid), 1)
    )
    mine = jnp.where(mine, 1.0, 0.0).astype(jnp.bfloat16)
    self_rows = dot(mine, selfw[...], 1, 1).astype(jnp.bfloat16)
    neigh_rows = dot(mine, neighw[...], 1, 1).astype(jnp.bfloat16)

    local_sum = dot(hidden, counts[0:nodes, :], 1, 0)

    def arrive(step, carry):
        to_part(step).wait_recv()
        return carry

    lax.fori_loop(1, parts, arrive, 0)

    half = lax.broadcasted_iota(jnp.int32, (short, LANES), 1) // capacity

    def unpack(index, carry):
        for piece in range(fold):
            value = jnp.zeros((short, LANES), jnp.float32)
            for place in range(fold):
                block = packed_in[index * fold + place].astype(jnp.float32)
                shift = (place - piece) * capacity % LANES
                if shift:
                    block = pltpu.roll(block, shift, 1)
                value = jnp.where(half == place, block, value)
            table[piece * short : (piece + 1) * short, pl.ds(pl.multiple_of(index * LANES, LANES), LANES)] = (
                value.astype(jnp.bfloat16)
            )
        return carry

    lax.fori_loop(0, parts // fold, unpack, 0)
    summed = local_sum + dot(table[...], counts[nodes:, :], 1, 0)
    mean_all[band(column), :] = (summed / degree[...].astype(jnp.float32)).astype(jnp.bfloat16)
    mean_copies = share(mean_all, mean_send, mean_recv)
    for copy in mean_copies:
        copy.start()
    for copy in hidden_copies:
        copy.wait_recv()
    result = dot(self_rows, hidden_all[...], 1, 0)
    for copy in mean_copies:
        copy.wait_recv()
    result = result + dot(neigh_rows, mean_all[...], 1, 0)
    out_ref[...] = jnp.maximum(result, 0.0).astype(out_ref.dtype)

    for copy in sums + hidden_copies + mean_copies:
        copy.wait_send()

    def sent(step, carry):
        to_part(step).wait_send()
        return carry

    lax.fori_loop(1, parts, sent, 0)


def local(features, proj_in, self_weight, neigh_weight, neighbors, degree, send_rows, send_count):
    cols = lax.axis_size("cols")
    parts = lax.axis_size("dom")
    hid = proj_in.shape[1]
    width = hid // cols
    nodes = features.shape[1]
    slots = send_rows.shape[1]
    capacity = slots // parts
    fold = LANES // capacity
    short = width // fold
    degree = degree.reshape(1, nodes)
    arguments = (
        features,
        proj_in,
        self_weight,
        neigh_weight,
        neighbors,
        degree,
        send_rows,
        send_count,
    )
    bf16 = jnp.bfloat16
    copies = pltpu.SemaphoreType.DMA
    return pl.pallas_call(
        functools.partial(kernel, cols, parts, capacity),
        out_shape=jax.ShapeDtypeStruct((width, nodes), bf16),
        in_specs=[pl.BlockSpec(memory_space=pltpu.HBM)] * len(arguments),
        out_specs=pl.BlockSpec(memory_space=pltpu.VMEM),
        scratch_shapes=[pltpu.VMEM(a.shape, a.dtype) for a in arguments]
        + [
            pltpu.VMEM((hid, nodes), jnp.float32),
            pltpu.VMEM((hid, nodes), bf16),
            pltpu.VMEM((cols - 1, width, nodes), bf16),
            pltpu.VMEM((hid, nodes), bf16),
            pltpu.VMEM((hid, nodes), bf16),
            pltpu.VMEM((nodes, slots * fold), bf16),
            pltpu.VMEM((parts, short, LANES), bf16),
            pltpu.VMEM((parts, short, LANES), bf16),
            pltpu.VMEM((width, slots), bf16),
            pltpu.VMEM((nodes + slots, nodes), bf16),
            copies((len(arguments),)),
            copies((cols - 1,)),
            copies((cols - 1,)),
            copies((parts,)),
            copies((parts,)),
            copies((cols - 1,)),
            copies((cols - 1,)),
            copies((cols - 1,)),
            copies((cols - 1,)),
        ],
        compiler_params=pltpu.CompilerParams(
            collective_id=0, has_side_effects=True, vmem_limit_bytes=67043328
        ),
        name="layer",
    )(*arguments)


def solution(mesh):
    return jax.shard_map(
        local,
        mesh=mesh,
        in_specs=(
            P("cols", "dom"),
            P("cols", None),
            P(),
            P(),
            P(None, "dom"),
            P("dom"),
            P("dom", None),
            P("dom", None),
        ),
        out_specs=P("cols", "dom"),
        check_vma=False,
    )
```

```python
import functools
import math

import jax
import jax.numpy as jnp
from jax import lax
from jax.experimental import pallas as pl
from jax.experimental.pallas import tpu as pltpu
from jax.sharding import PartitionSpec as P

MESH = pl.DeviceIdType.MESH
LANES = 128


def dot(left, right, left_dim, right_dim):
    return lax.dot_general(
        left, right, (((left_dim,), (right_dim,)), ((), ())), preferred_element_type=jnp.float32
    )


def kernel(
    cols,
    parts,
    capacity,
    feat_hbm,
    proj_hbm,
    selfw_hbm,
    neighw_hbm,
    neigh_hbm,
    degree_hbm,
    rows_hbm,
    count_hbm,
    out_ref,
    feat,
    proj,
    selfw,
    neighw,
    neigh,
    degree,
    rows,
    count,
    own,
    outgoing_sum,
    incoming_sum,
    hidden_all,
    pick,
    packed_out,
    packed_in,
    table,
    counts,
    in_sem,
    sum_send,
    sum_recv,
    row_send,
    row_recv,
    hid_send,
    hid_recv,
    pass_send,
    pass_recv,
):
    column = lax.axis_index("cols")
    part = lax.axis_index("dom")
    width = out_ref.shape[0]
    nodes = out_ref.shape[1]
    hid = width * cols
    slots = rows.shape[1]
    slot_count = neigh.shape[0]
    fold = LANES // capacity
    short = width // fold

    loads = [
        pltpu.make_async_copy(source, target, in_sem.at[i])
        for i, (source, target) in enumerate(
            (
                (feat_hbm, feat),
                (proj_hbm, proj),
                (rows_hbm, rows),
                (count_hbm, count),
                (neigh_hbm, neigh),
                (degree_hbm, degree),
                (selfw_hbm, selfw),
                (neighw_hbm, neighw),
            )
        )
    ]
    for load in loads:
        load.start()

    barrier = pltpu.get_barrier_semaphore()
    for step in range(1, cols):
        pl.semaphore_signal(
            barrier, inc=1, device_id=((column + step) % cols, part), device_id_type=MESH
        )

    def greet(step, carry):
        pl.semaphore_signal(
            barrier, inc=1, device_id=(column, (part + step) % parts), device_id_type=MESH
        )
        return carry

    lax.fori_loop(1, parts, greet, 0)

    loads[0].wait()
    loads[1].wait()
    partial_value = dot(proj[...], feat[...], 0, 0)
    own[...] = partial_value
    outgoing_sum[...] = partial_value.astype(outgoing_sum.dtype)
    pl.semaphore_wait(barrier, cols + parts - 2)

    def band(index):
        return pl.ds(pl.multiple_of(index * width, width), width)

    def to_column(source, target, send, recv, step):
        peer = (column + step) % cols
        return pltpu.make_async_remote_copy(
            src_ref=source,
            dst_ref=target,
            send_sem=send.at[step - 1],
            recv_sem=recv.at[step - 1],
            device_id=(peer, part),
            device_id_type=MESH,
        )

    sums = [
        to_column(
            outgoing_sum.at[band((column + step) % cols)],
            incoming_sum.at[step - 1],
            sum_send,
            sum_recv,
            step,
        )
        for step in range(1, cols)
    ]
    for copy in sums:
        copy.start()

    for load in loads[2:6]:
        load.wait()
    group = min(slots, 512)
    spread = group * fold

    def choose(index, carry):
        start = pl.multiple_of(index * group, group)
        wanted = rows[:, pl.ds(start, group)]
        source = (
            lax.broadcasted_iota(jnp.int32, (parts, group), 1) + start
        ) // capacity == lax.broadcasted_iota(jnp.int32, (parts, group), 0)
        amount = dot(
            jnp.broadcast_to(count[...].astype(jnp.float32), (8, parts)).astype(jnp.bfloat16),
            source.astype(jnp.float32).astype(jnp.bfloat16),
            1,
            0,
        )[0:1, :]
        slot = (lax.broadcasted_iota(jnp.int32, (1, group), 1) % capacity).astype(jnp.float32)
        wanted = jnp.where(slot < amount, wanted, -1)
        pieces = []
        for block in range(group // capacity):
            piece = wanted[:, block * capacity : (block + 1) * capacity]
            pieces += [piece] * fold
        wide = jnp.concatenate(pieces, axis=1)
        hit = lax.broadcasted_iota(jnp.int32, (nodes, spread), 0) == wide
        pick[:, pl.ds(pl.multiple_of(index * spread, spread), spread)] = jnp.where(
            hit, 1.0, 0.0
        ).astype(jnp.bfloat16)
        return carry

    lax.fori_loop(0, slots // group, choose, 0)

    used = lax.broadcasted_iota(jnp.int32, (slot_count, nodes), 0) < degree[...]
    codes = jnp.where(used, neigh[...], -1)
    neigh[...] = codes
    depth = 256
    row_of = lax.broadcasted_iota(jnp.int32, (depth, LANES), 0).astype(jnp.float32).astype(jnp.bfloat16)
    one = jnp.ones((depth, LANES), jnp.bfloat16)
    zero = jnp.zeros((depth, LANES), jnp.bfloat16)

    def tally(index, carry):
        start = pl.multiple_of(index * depth, depth)
        for lane in range(nodes // LANES):
            there = slice(lane * LANES, (lane + 1) * LANES)
            near = jnp.clip(neigh[:, there] - start, -1, depth).astype(jnp.float32)
            total = zero
            for slot in range(slot_count):
                code = jnp.broadcast_to(near[slot : slot + 1, :], (16, LANES)).astype(jnp.bfloat16)
                code = jnp.concatenate([code] * (depth // 16), axis=0)
                total = total + jnp.where(row_of == code, one, zero)
            counts[pl.ds(start, depth), there] = total
        return carry

    lax.fori_loop(0, nodes // depth, tally, 0)

    total = own[band(column), :]
    for step in range(1, cols):
        sums[step - 1].wait_recv()
    for step in range(1, cols):
        total = total + incoming_sum[step - 1].astype(jnp.float32)
    hidden = total.astype(jnp.bfloat16)
    hidden_all[band(column), :] = hidden

    folded = lax.broadcasted_iota(jnp.int32, (short, spread), 1) % LANES // capacity

    def pack(index, carry):
        start = pl.multiple_of(index * spread, spread)
        chosen = dot(hidden_all[band(column), :], pick[:, pl.ds(start, spread)], 1, 0)
        tight = chosen[0:short, :]
        for piece in range(1, fold):
            tight = jnp.where(folded == piece, chosen[piece * short : (piece + 1) * short, :], tight)
        tight = tight.astype(jnp.bfloat16)
        for block in range(spread // LANES):
            packed_out[index * (spread // LANES) + block] = tight[:, block * LANES : (block + 1) * LANES]
        return carry

    lax.fori_loop(0, slots // group, pack, 0)

    def to_part(step):
        peer = (part + step) % parts
        return pltpu.make_async_remote_copy(
            src_ref=packed_out.at[peer],
            dst_ref=packed_in.at[column, part],
            send_sem=row_send.at[step],
            recv_sem=row_recv.at[step],
            device_id=(column, peer),
            device_id_type=MESH,
        )

    def send_rows(step, carry):
        to_part(step).start()
        return carry

    lax.fori_loop(1, parts, send_rows, 0)

    def share(buffer, send, recv):
        return [
            to_column(buffer.at[band(column)], buffer.at[band(column)], send, recv, step)
            for step in range(1, cols)
        ]

    hidden_copies = share(hidden_all, hid_send, hid_recv)
    for copy in hidden_copies:
        copy.start()

    for index in range(cols):
        packed_in[index, part] = jnp.zeros((short, LANES), jnp.bfloat16)
    lax.fori_loop(nodes // depth, counts.shape[0] // depth, tally, 0)
    for load in loads[6:]:
        load.wait()
    mine = (
        lax.broadcasted_iota(jnp.int32, (width, hid), 0) + column * width
        == lax.broadcasted_iota(jnp.int32, (width, hid), 1)
    )
    mine = jnp.where(mine, 1.0, 0.0).astype(jnp.bfloat16)
    self_rows = dot(mine, selfw[...], 1, 1).astype(jnp.bfloat16)
    neigh_rows = dot(mine, neighw[...], 1, 1).astype(jnp.bfloat16)

    def forward(step, source):
        return to_column(
            packed_in.at[column, source],
            packed_in.at[column, source],
            pass_send.at[source],
            pass_recv.at[source],
            step,
        )

    def arrive(step, carry):
        to_part(step).wait_recv()
        for hop in range(1, cols):
            forward(hop, (part - step + parts) % parts).start()
        return carry

    lax.fori_loop(1, parts, arrive, 0)
    for copy in hidden_copies:
        copy.wait_recv()
    own[...] = dot(hidden_all[...], counts[0:nodes, :], 1, 0)

    def passed(step, carry):
        for hop in range(1, cols):
            forward(hop, (part - step + parts) % parts).wait_recv()
        return carry

    lax.fori_loop(1, parts, passed, 0)

    half = lax.broadcasted_iota(jnp.int32, (short, LANES), 1) // capacity

    def unpack(index, carry):
        columns = pl.ds(pl.multiple_of(index * LANES, LANES), LANES)
        for source in range(cols):
            for piece in range(fold):
                value = jnp.zeros((short, LANES), jnp.float32)
                for place in range(fold):
                    block = packed_in[source, index * fold + place].astype(jnp.float32)
                    shift = (place - piece) * capacity % LANES
                    if shift:
                        block = pltpu.roll(block, shift, 1)
                    value = jnp.where(half == place, block, value)
                start = source * width + piece * short
                table[start : start + short, columns] = value.astype(jnp.bfloat16)
        return carry

    lax.fori_loop(0, parts // fold, unpack, 0)
    summed = own[...] + dot(table[...], counts[nodes:, :], 1, 0)
    mean = (summed / degree[...].astype(jnp.float32)).astype(jnp.bfloat16)
    result = dot(self_rows, hidden_all[...], 1, 0) + dot(neigh_rows, mean, 1, 0)
    out_ref[...] = jnp.maximum(result, 0.0).astype(out_ref.dtype)

    for copy in sums + hidden_copies:
        copy.wait_send()

    def sent(step, carry):
        to_part(step).wait_send()
        for hop in range(1, cols):
            forward(hop, (part - step + parts) % parts).wait_send()
        return carry

    lax.fori_loop(1, parts, sent, 0)


def local(features, proj_in, self_weight, neigh_weight, neighbors, degree, send_rows, send_count):
    cols = lax.axis_size("cols")
    parts = lax.axis_size("dom")
    hid = proj_in.shape[1]
    width = hid // cols
    nodes = features.shape[1]
    slots = send_rows.shape[1]
    capacity = slots // parts
    fold = LANES // capacity
    short = width // fold
    degree = degree.reshape(1, nodes)
    arguments = (
        features,
        proj_in,
        self_weight,
        neigh_weight,
        neighbors,
        degree,
        send_rows,
        send_count,
    )
    bf16 = jnp.bfloat16
    copies = pltpu.SemaphoreType.DMA
    return pl.pallas_call(
        functools.partial(kernel, cols, parts, capacity),
        out_shape=jax.ShapeDtypeStruct((width, nodes), bf16),
        in_specs=[pl.BlockSpec(memory_space=pltpu.HBM)] * len(arguments),
        out_specs=pl.BlockSpec(memory_space=pltpu.VMEM),
        scratch_shapes=[pltpu.VMEM(a.shape, a.dtype) for a in arguments]
        + [
            pltpu.VMEM((hid, nodes), jnp.float32),
            pltpu.VMEM((hid, nodes), bf16),
            pltpu.VMEM((cols - 1, width, nodes), bf16),
            pltpu.VMEM((hid, nodes), bf16),
            pltpu.VMEM((nodes, slots * fold), bf16),
            pltpu.VMEM((parts, short, LANES), bf16),
            pltpu.VMEM((cols, parts, short, LANES), bf16),
            pltpu.VMEM((hid, slots), bf16),
            pltpu.VMEM((nodes + slots, nodes), bf16),
            copies((len(arguments),)),
            copies((cols - 1,)),
            copies((cols - 1,)),
            copies((parts,)),
            copies((parts,)),
            copies((cols - 1,)),
            copies((cols - 1,)),
            copies((parts, cols - 1)),
            copies((parts, cols - 1)),
        ],
        compiler_params=pltpu.CompilerParams(
            collective_id=0, has_side_effects=True, vmem_limit_bytes=67043328
        ),
        name="layer",
    )(*arguments)


def solution(mesh):
    return jax.shard_map(
        local,
        mesh=mesh,
        in_specs=(
            P("cols", "dom"),
            P("cols", None),
            P(),
            P(),
            P(None, "dom"),
            P("dom"),
            P("dom", None),
            P("dom", None),
        ),
        out_specs=P("cols", "dom"),
        check_vma=False,
    )
```
